32 devices in a mesh: node: 8 (over z, core), group: 4 (over y, x).
Axes of the slice: x: 2, y: 2, z: 4, core: 2. Of those that a mesh axis runs over, the one named last changes fastest.
Arguments:
- gradient: bfloat16 [8, 4, 128, 1024], P('node', 'group'), may hold values from -60 to 60
- momentum: float32 [128, 1024], replicated, may hold values from -6 to 6
- variance: float32 [128, 1024], replicated, may hold values from 0.004 to 0.4
- params: float32 [128, 1024], replicated, may hold values from -6 to 6
- worker_error: float32 [8, 4, 128, 1024], P('node', 'group'), may hold values from -18 to 18, as said below
- server_error: float32 [4, 128, 1024], P('group', 'node'), may hold values from -12 to 12, as said below
- group_worker_error: float32 [4, 128, 1024], P('group', 'node'), may hold values from -12 to 12, as said below
- group_server_error: float32 [128, 1024], P(('node', 'group')), may hold values from -12 to 12, as said below
Outputs:
- new_params: float32 [128, 1024], replicated
- new_momentum: float32 [128, 1024], replicated
- new_worker_error: float32 [8, 4, 128, 1024], P('node', 'group')
- new_server_error: float32 [4, 128, 1024], P('group', 'node')
- new_group_worker_error: float32 [4, 128, 1024], P('group', 'node')
- new_group_server_error: float32 [128, 1024], P(('node', 'group'))
The draws below stay inside these ranges and needn't reach their ends.
Inputs may be any that keep to these rules, and one draw needn't show every extreme that they name: `worker_error`: no entry of local has magnitude under 0.005. No entry of group_mean + server_error has magnitude under 0.005. No entry of group_q + group_worker_error has magnitude under 0.005. No entry of total_mean + group_server_error has magnitude under 0.005.
All inputs are finite; a program needn't handle non-finite values.
Results may differ from the reference program's by a relative error of at most 0.0003.
Values sent between devices are 32-bit elements; how exact they have to be, the bound alone decides.
No kernel may reach another device: no remote copies, remote signals or barrier semaphores. Data moves between devices by JAX's collectives and lax.ppermute only.
A program may use at most 128 MiB of HBM per device.

```python
import math
import jax
import jax.numpy as jnp
from jax import lax

D = 1024
PIECE_ROWS = 4
ROWS = 128
N_NODE = 8
N_GROUP = 4


def compress_draw(values):
    scale = jnp.mean(jnp.abs(values), axis=-1, keepdims=True)
    return scale * jnp.sign(values)


def signed_draw(key, shape, lower, upper):
    first_key, second_key = jax.random.split(key)
    magnitude = jax.random.uniform(first_key, shape, jnp.float32, lower, upper)
    flips = jax.random.bernoulli(second_key, 0.5, shape)
    return jnp.where(flips, magnitude, -magnitude)


def leaning_target(key, shape, leaning):
    first_key, second_key = jax.random.split(key)
    magnitude = jax.random.uniform(first_key, shape, jnp.float32, 0.1, 0.6)
    agrees = jax.random.bernoulli(second_key, 0.75, shape)
    return jnp.where(agrees, 1.0, -1.0) * leaning * magnitude


def joint_state(key):
    total_rows = PIECE_ROWS * N_NODE * N_GROUP
    base = jax.random.fold_in(key, 101)
    keys = [jax.random.fold_in(base, index) for index in range(8)]
    momentum = jax.random.uniform(keys[2], (total_rows, D), jnp.float32, -0.6, 0.6)
    leaning = jnp.where(momentum >= 0.0, 1.0, -1.0)
    gradient = signed_draw(keys[3], (N_NODE, N_GROUP, total_rows, D), 2.0, 6.0)
    gradient = gradient.astype(jnp.bfloat16)
    moved = 0.9 * momentum + 0.1 * gradient.astype(jnp.float32)
    local_target = leaning_target(keys[4], (N_NODE, N_GROUP, total_rows, D), leaning)
    worker_error = local_target - moved
    first = compress_draw(moved + worker_error)
    group_mean = jnp.sum(first, axis=0) / N_NODE
    server_target = leaning_target(keys[5], (N_GROUP, total_rows, D), leaning)
    server_error = server_target - group_mean
    group_q = compress_draw(group_mean + server_error)
    second_target = leaning_target(keys[6], (N_GROUP, total_rows, D), leaning)
    group_worker_error = second_target - group_q
    second = compress_draw(group_q + group_worker_error)
    total_mean = jnp.sum(second, axis=0) / N_GROUP
    last_target = leaning_target(keys[7], (total_rows, D), leaning)
    group_server_error = last_target - total_mean
    return (momentum, gradient, worker_error, server_error, group_worker_error, group_server_error)


def draw_gradient(key, part):
    return joint_state(key)[1]


def draw_momentum(key, part):
    return joint_state(key)[0]


def draw_worker_error(key, part):
    return joint_state(key)[2]


def draw_server_error(key, part):
    return joint_state(key)[3]


def draw_group_worker_error(key, part):
    return joint_state(key)[4]


def draw_group_server_error(key, part):
    return joint_state(key)[5]


def bell_draw(rng, dims, scale, most, kind=jnp.bfloat16):
    result = scale * jax.random.normal(rng, dims, jnp.float32)
    return jnp.clip(result, min=-most, max=most).astype(kind)


def setup_inputs(seed: int = 0) -> dict:
    key_list = jax.random.split(jax.random.key(seed), 9)
    return {
        "gradient": draw_gradient(jax.random.fold_in(key_list[8], 71), 0),
        "momentum": draw_momentum(jax.random.fold_in(key_list[8], 71), 0),
        "variance": jnp.clip(jnp.exp(jax.random.uniform(key_list[2], (ROWS, D), jnp.float32, math.log(0.004), math.log(0.4))), 0.004, 0.4),
        "params": bell_draw(key_list[3], (ROWS, D), 1.0, 6.0, jnp.float32),
        "worker_error": draw_worker_error(jax.random.fold_in(key_list[8], 71), 0),
        "server_error": draw_server_error(jax.random.fold_in(key_list[8], 71), 0),
        "group_worker_error": draw_group_worker_error(jax.random.fold_in(key_list[8], 71), 0),
        "group_server_error": draw_group_server_error(jax.random.fold_in(key_list[8], 71), 0),
    }


def compress(values):
    scale = lax.optimization_barrier(jnp.mean(jnp.abs(values), axis=-1, keepdims=True))
    packed = scale * jnp.sign(values)
    return (packed, values - packed)

def reference(gradient, momentum, variance, params, worker_error, server_error, group_worker_error, group_server_error):
    local = 0.9 * momentum + 0.1 * gradient.astype(jnp.float32) + worker_error
    first, new_worker_error = compress(local)
    group_mean = lax.optimization_barrier(jnp.sum(first, axis=0)) / N_NODE
    group_q, new_server_error = compress(group_mean + server_error)
    second, new_group_worker_error = compress(group_q + group_worker_error)
    total_mean = lax.optimization_barrier(jnp.sum(second, axis=0)) / N_GROUP
    new_momentum, new_group_server_error = compress(total_mean + group_server_error)
    new_params = params - 0.05 * new_momentum / (jnp.sqrt(variance) + 1e-08)
    return (new_params, new_momentum, new_worker_error, new_server_error, new_group_worker_error, new_group_server_error)
```

```python
import jax
import jax.numpy as jnp
from jax import lax
from jax.sharding import PartitionSpec as P

CORES = 2


def compress(values):
    scale = jnp.mean(jnp.abs(values), axis=-1, keepdims=True)
    packed = scale * jnp.sign(values)
    return (packed, values - packed)


def partner(index, step, size):
    if size & (size - 1) == 0:
        return index ^ step
    return (index + step) % size


def source(index, step, size):
    if size & (size - 1) == 0:
        return index ^ step
    return (index - step + size) % size


def swap_cores(values, nodes):
    return lax.ppermute(values, "node", [(i, i ^ 1) for i in range(nodes)])


def send_chip(values, step, nodes):
    chips = nodes // CORES
    pairs = [
        (chip * CORES + core, partner(chip, step, chips) * CORES + core)
        for chip in range(chips)
        for core in range(CORES)
    ]
    return lax.ppermute(values, "node", pairs)


def send_group(values, step, groups):
    return lax.ppermute(values, "group", [(i, partner(i, step, groups)) for i in range(groups)])


def pick(blocks, index, axis=0):
    return lax.dynamic_index_in_dim(blocks, index, axis, keepdims=False)


def place(blocks, value, index, axis):
    return lax.dynamic_update_index_in_dim(blocks, value, index, axis)


def body(
    gradient,
    momentum,
    variance,
    params,
    worker_error,
    server_error,
    group_worker_error,
    group_server_error,
):
    nodes = lax.axis_size("node")
    groups = lax.axis_size("group")
    chips = nodes // CORES
    rows, width = momentum.shape
    shard_rows = rows // nodes
    node = lax.axis_index("node")
    group = lax.axis_index("group")
    chip, core = node // CORES, node % CORES

    piece_rows = group_server_error.shape[0]
    pieces = jnp.zeros((groups, piece_rows, width), jnp.float32)
    pieces = place(pieces, group_server_error, group, 0)
    for step in range(1, groups):
        pieces = place(pieces, send_group(group_server_error, step, groups), source(group, step, groups), 0)
    shard_server_error = pieces.reshape(shard_rows, width)

    local = 0.9 * momentum + 0.1 * gradient[0, 0].astype(jnp.float32) + worker_error[0, 0]
    first, new_worker_error = compress(local)

    blocks = first.reshape(chips, CORES, shard_rows, width)
    kept, given = pick(blocks, core, 1), pick(blocks, 1 - core, 1)
    chip_sum = kept + swap_cores(given, nodes)
    total = pick(chip_sum, chip)
    for step in range(1, chips):
        total = total + send_chip(pick(chip_sum, partner(chip, step, chips)), step, nodes)
    group_mean = total / nodes

    group_q, new_server_error = compress(group_mean + server_error[0])
    second, new_group_worker_error = compress(group_q + group_worker_error[0])

    total = second
    for step in range(1, groups):
        total = total + send_group(second, step, groups)
    total_mean = total / groups
    shard_momentum, shard_error = compress(total_mean + shard_server_error)
    new_group_server_error = pick(shard_error.reshape(groups, piece_rows, width), group)

    mine = jnp.zeros((chips, shard_rows, width), jnp.float32)
    mine = place(mine, shard_momentum, chip, 0)
    for step in range(1, chips):
        mine = place(mine, send_chip(shard_momentum, step, nodes), source(chip, step, chips), 0)
    other = swap_cores(mine, nodes)
    both = jnp.where(core == 0, jnp.stack([mine, other], 1), jnp.stack([other, mine], 1))
    new_momentum = both.reshape(rows, width)
    new_params = params - 0.05 * new_momentum / (jnp.sqrt(variance) + 1e-08)
    return (
        new_params,
        new_momentum,
        new_worker_error[None, None],
        new_server_error[None],
        new_group_worker_error[None],
        new_group_server_error,
    )


def solution(mesh):
    in_specs = (
        P("node", "group", None, None),
        P(),
        P(),
        P(),
        P("node", "group", None, None),
        P("group", "node", None),
        P("group", "node", None),
        P(("node", "group"), None),
    )
    out_specs = (
        P(),
        P(),
        P("node", "group", None, None),
        P("group", "node", None),
        P("group", "node", None),
        P(("node", "group"), None),
    )
    return jax.shard_map(body, mesh=mesh, in_specs=in_specs, out_specs=out_specs, check_vma=False)
```

```python
import functools

import jax
import jax.numpy as jnp
from jax import lax
from jax.experimental import pallas as pl
from jax.experimental.pallas import tpu as pltpu
from jax.sharding import PartitionSpec as P

CORES = 2
VMEM = pl.BlockSpec(memory_space=pltpu.VMEM)
HBM = pl.BlockSpec(memory_space=pltpu.HBM)


def paired(size):
    return size & (size - 1) == 0


def target(index, step, size):
    if paired(size):
        return index ^ step
    return lax.rem(index + step, size) if not isinstance(index, int) else (index + step) % size


def source(index, step, size):
    return index ^ step if paired(size) else lax.rem(index + (size - step), size)


def steps_of(size):
    if not paired(size):
        return list(range(1, size))
    steps, half = [], size // 2
    while half:
        steps += range(half, 2 * half)
        half //= 2
    return steps


def packed_of(values, width):
    scale = jnp.sum(jnp.abs(values), axis=-1, keepdims=True) / width
    return jnp.where(values > 0, scale, jnp.where(values < 0, -scale, jnp.zeros_like(values)))


def swap_cores(values, nodes):
    return lax.ppermute(values, "node", [(i, i ^ 1) for i in range(nodes)])


def send_chip(values, step, nodes):
    chips = nodes // CORES
    pairs = [
        (CORES * i + core, CORES * target(i, step, chips) + 1 - core) for i in range(chips) for core in range(CORES)
    ]
    return lax.ppermute(values, "node", pairs)


def send_group(values, step, groups):
    return lax.ppermute(values, "group", [(i, target(i, step, groups)) for i in range(groups)])


def vmem(*shape):
    return pltpu.VMEM(shape, jnp.float32)


def near(*values):
    return [pltpu.with_memory_space_constraint(value, pltpu.VMEM) for value in values]


def far(*values):
    return [pltpu.with_memory_space_constraint(value, pltpu.HBM) for value in values]


def room(*scratch):
    return pltpu.CompilerParams(vmem_limit_bytes=sum(scratch) + (4 << 20))


def place_of():
    node = lax.axis_index("node")
    return node // CORES, lax.rem(node, CORES)


def head_kernel(order, gradient, momentum, worker_error, *rest):
    chips = len(order)
    small, rest = rest[:3], rest[3:]
    kept, (sooner, later, error, *near_small, g_buf, m_buf, w_buf, sems, small_sems) = rest[:chips], rest[chips:]
    rows, width = momentum.shape
    chip_rows = rows // chips
    shard_rows = chip_rows // CORES
    chip, core = place_of()
    copies = []
    for at, step in enumerate(order):
        where = target(chip, step, chips)
        part = pl.ds(pl.multiple_of(where * chip_rows, chip_rows), chip_rows)
        pairs = ((gradient.at[0, 0], g_buf), (momentum, m_buf), (worker_error.at[0, 0], w_buf))
        three = [
            pltpu.make_async_copy(src.at[part], dst.at[at], sems.at[at, kind]) for kind, (src, dst) in enumerate(pairs)
        ]
        for copy in three:
            copy.start()
        copies.append((where, three))
    brought = [pltpu.make_async_copy(src, dst, small_sems.at[i]) for i, (src, dst) in enumerate(zip(small, near_small))]
    for copy in brought:
        copy.start()
    for at, (where, three) in enumerate(copies):
        for copy in three:
            copy.wait()
        mine = core if order[at] == 0 else 1 - core
        for side, half in enumerate((mine, 1 - mine)):
            some = pl.ds(pl.multiple_of(half * shard_rows, shard_rows), shard_rows)
            local = 0.9 * m_buf[at, some] + 0.1 * g_buf[at, some].astype(jnp.float32) + w_buf[at, some]
            first = packed_of(local, width)
            if side == 0:
                kept[at][...] = first
            elif at == 0:
                sooner[...] = first
            else:
                later[at - 1] = first
            start = pl.multiple_of(where * chip_rows + half * shard_rows, shard_rows)
            error[pl.ds(start, shard_rows), :] = local - first
    for copy in brought:
        copy.wait()


def head(gradient, momentum, worker_error, small, order):
    rows, width = momentum.shape
    chips = len(order)
    chip_rows = rows // chips
    shard = (chip_rows // CORES, width)
    return pl.pallas_call(
        functools.partial(head_kernel, order),
        out_shape=[vmem(*shard)] * (chips + 1) + [vmem(chips - 1, *shard), vmem(rows, width)] + [vmem(*x.shape) for x in small],
        in_specs=[HBM] * 6,
        out_specs=[VMEM] * (chips + 6),
        scratch_shapes=[
            pltpu.VMEM((chips, chip_rows, width), gradient.dtype),
            pltpu.VMEM((chips, chip_rows, width), jnp.float32),
            pltpu.VMEM((chips, chip_rows, width), jnp.float32),
            pltpu.SemaphoreType.DMA((chips, 3)),
            pltpu.SemaphoreType.DMA((3,)),
        ],
        compiler_params=room(gradient.nbytes, momentum.nbytes, worker_error.nbytes),
    )(*far(gradient, momentum, worker_error, *small))


def server_kernel(nodes, count, *refs):
    parts, (server, worker, second, error_0, error_1) = refs[:count], refs[count:]
    width = server.shape[-1]
    total = parts[0][...]
    for other in parts[1:]:
        total = total + other[...]
    values = total / nodes + server[...]
    group_q = packed_of(values, width)
    error_0[...] = values - group_q
    values = group_q + worker[...]
    result = packed_of(values, width)
    second[...] = result
    error_1[...] = values - result


def serve(parts, server, worker, nodes):
    return pl.pallas_call(
        functools.partial(server_kernel, nodes, len(parts)),
        out_shape=[vmem(*server.shape)] * 3,
        in_specs=[VMEM] * (len(parts) + 2),
        out_specs=[VMEM] * 3,
        compiler_params=room(),
    )(*near(*parts, server, worker))


def store_kernel(count, *refs):
    sems = refs[-1]
    copies = [pltpu.make_async_copy(refs[i], refs[count + i], sems.at[i]) for i in range(count)]
    for copy in copies:
        copy.start()
    for copy in copies:
        copy.wait()


def store(*values):
    count = len(values)
    return pl.pallas_call(
        functools.partial(store_kernel, count),
        out_shape=[pltpu.HBM(value.shape, jnp.float32) for value in values],
        in_specs=[VMEM] * count,
        out_specs=[HBM] * count,
        scratch_shapes=[pltpu.SemaphoreType.DMA((count,))],
        compiler_params=room(),
    )(*near(*values))


def average_kernel(groups, *refs):
    parts, (server, result, error) = refs[:groups], refs[groups:]
    width = server.shape[-1]
    total = parts[0][...]
    for other in parts[1:]:
        total = total + other[...]
    values = total / groups + server[...]
    packed = packed_of(values, width)
    result[...] = packed
    error[...] = values - packed


def average(parts, server):
    return pl.pallas_call(
        functools.partial(average_kernel, len(parts)),
        out_shape=[vmem(*server.shape)] * 2,
        in_specs=[VMEM] * (len(parts) + 1),
        out_specs=[VMEM] * 2,
        compiler_params=room(),
    )(*near(*parts, server))


def update_kernel(steps, chips, *refs):
    count = len(steps)
    mine, given, (variance, params) = refs[:count], refs[count : 2 * count], refs[2 * count : 2 * count + 2]
    new_params, new_momentum, p_buf, m_buf, sems = refs[-5:]
    shard_rows = mine[0].shape[0]
    chip_rows = CORES * shard_rows
    chip, core = place_of()
    copies = []
    for at, step in enumerate(steps):
        part = pl.ds(pl.multiple_of(source(chip, step, chips) * chip_rows, chip_rows), chip_rows)
        half = core if step == 0 else 1 - core
        for values, side in ((mine[at], half), (given[at], 1 - half)):
            m_buf[at, pl.ds(pl.multiple_of(side * shard_rows, shard_rows), shard_rows), :] = values[...]
        copies.append(pltpu.make_async_copy(m_buf.at[at], new_momentum.at[part], sems.at[at, 0]))
        copies[-1].start()
        p_buf[at] = params[part, :] - 0.05 * m_buf[at] / (jnp.sqrt(variance[part, :]) + 1e-08)
        copies.append(pltpu.make_async_copy(p_buf.at[at], new_params.at[part], sems.at[at, 1]))
        copies[-1].start()
    for copy in copies:
        copy.wait()


def update(mine, given, variance, params, so_far, steps, chips):
    shard_rows, width = mine[0].shape
    count = len(steps)
    buffer = (count, CORES * shard_rows, width)
    return pl.pallas_call(
        functools.partial(update_kernel, steps, chips),
        out_shape=[pltpu.HBM(params.shape, jnp.float32)] * 2,
        in_specs=[VMEM] * (2 * count + 2) + [HBM] * len(so_far),
        out_specs=[HBM] * 2,
        scratch_shapes=[
            pltpu.VMEM(buffer, jnp.float32),
            pltpu.VMEM(buffer, jnp.float32),
            pltpu.SemaphoreType.DMA((count, 2)),
        ],
        input_output_aliases={2 * count + 2 + i: i for i in range(len(so_far))},
        compiler_params=room(2 * count * CORES * mine[0].nbytes),
    )(*near(*mine, *given, variance, params), *so_far)


def body(
    gradient,
    momentum,
    variance,
    params,
    worker_error,
    server_error,
    group_worker_error,
    group_server_error,
):
    nodes = lax.axis_size("node")
    groups = lax.axis_size("group")
    chips = nodes // CORES
    rows, width = momentum.shape
    shard_rows = rows // nodes
    piece_rows = group_server_error.shape[0]
    group = lax.axis_index("group")
    along = steps_of(chips)
    across = steps_of(groups)

    small = (server_error[0], group_worker_error[0], group_server_error)
    *kept, sooner, later, error, server, worker, own_piece = head(gradient, momentum, worker_error, small, along + [0])
    got = [swap_cores(sooner, nodes)]
    got += list(swap_cores(later, nodes))
    parts = [kept[-1], got[-1]]
    for at, step in enumerate(along):
        parts.append(send_chip(kept[at] + got[at], step, nodes))

    got_pieces = []
    for step in across:
        got_pieces.append(send_group(own_piece, step, groups))

    second, error_0, error_1 = serve(parts, server, worker, nodes)
    error_0, got_pieces = lax.optimization_barrier((error_0, got_pieces))
    pieces = jnp.zeros((groups, piece_rows, width), jnp.float32)
    for step, piece in zip([0] + across, [own_piece] + got_pieces):
        pieces = lax.dynamic_update_slice_in_dim(pieces, piece[None], source(group, step, groups), 0)
    seconds = [second]
    for step in across:
        seconds.append(send_group(second, step, groups))
    new_worker_error, new_server_error, new_group_worker_error = store(error[None, None], error_0[None], error_1[None])

    mine, shard_error = average(seconds, pieces.reshape(shard_rows, width))
    new_group_server_error = lax.dynamic_slice_in_dim(shard_error, group * piece_rows, piece_rows, 0)

    arrived = [mine]
    for step in along:
        arrived.append(send_chip(mine, step, nodes))
    given = []
    for step, values in zip([0] + along, arrived):
        given.append(swap_cores(values, nodes))
    outs = ()
    for some in (slice(0, 1), slice(1, chips - 1), slice(chips - 1, chips)):
        outs = update(arrived[some], given[some], variance, params, outs, ([0] + along)[some], chips)
    new_params, new_momentum = outs
    return (
        new_params,
        new_momentum,
        new_worker_error,
        new_server_error,
        new_group_worker_error,
        new_group_server_error,
    )


def solution(mesh):
    in_specs = (
        P("node", "group", None, None),
        P(),
        P(),
        P(),
        P("node", "group", None, None),
        P("group", "node", None),
        P("group", "node", None),
        P(("node", "group"), None),
    )
    out_specs = (
        P(),
        P(),
        P("node", "group", None, None),
        P("group", "node", None),
        P("group", "node", None),
        P(("node", "group"), None),
    )
    return jax.shard_map(body, mesh=mesh, in_specs=in_specs, out_specs=out_specs, check_vma=False)
```

```python
import functools

import jax
import jax.numpy as jnp
from jax import lax
from jax.experimental import pallas as pl
from jax.experimental.pallas import tpu as pltpu
from jax.sharding import PartitionSpec as P

CORES = 2
VMEM = pl.BlockSpec(memory_space=pltpu.VMEM)
HBM = pl.BlockSpec(memory_space=pltpu.HBM)


def paired(size):
    return size & (size - 1) == 0


def target(index, step, size):
    if paired(size):
        return index ^ step
    return lax.rem(index + step, size) if not isinstance(index, int) else (index + step) % size


def source(index, step, size):
    return index ^ step if paired(size) else lax.rem(index + (size - step), size)


def farthest_first(size):
    return list(range(size - 1, 0, -1))


def farthest_last(size):
    steps = farthest_first(size)
    return steps[1:] + steps[:1]


def packed_of(values, width):
    scale = jnp.sum(jnp.abs(values), axis=-1, keepdims=True) / width
    return jnp.where(values > 0, scale, jnp.where(values < 0, -scale, jnp.zeros_like(values)))


def swap_cores(values, nodes):
    return lax.ppermute(values, "node", [(i, i ^ 1) for i in range(nodes)])


def send_chip(values, step, nodes):
    chips = nodes // CORES
    pairs = [
        (CORES * i + core, CORES * target(i, step, chips) + 1 - core) for i in range(chips) for core in range(CORES)
    ]
    return lax.ppermute(values, "node", pairs)


def send_group(values, step, groups):
    return lax.ppermute(values, "group", [(i, target(i, step, groups)) for i in range(groups)])


def vmem(*shape):
    return pltpu.VMEM(shape, jnp.float32)


def near(*values):
    return [pltpu.with_memory_space_constraint(value, pltpu.VMEM) for value in values]


def far(*values):
    return [pltpu.with_memory_space_constraint(value, pltpu.HBM) for value in values]


def room(*scratch):
    return pltpu.CompilerParams(vmem_limit_bytes=sum(scratch) + (4 << 20))


def place_of():
    node = lax.axis_index("node")
    return node // CORES, lax.rem(node, CORES)


def head_kernel(order, gradient, momentum, worker_error, *rest):
    chips = len(order)
    small, rest = rest[:3], rest[3:]
    kept, (sooner, later, error, *near_small, g_buf, m_buf, w_buf, sems, small_sems) = rest[:chips], rest[chips:]
    rows, width = momentum.shape
    chip_rows = rows // chips
    shard_rows = chip_rows // CORES
    chip, core = place_of()
    copies = []
    for at, step in enumerate(order):
        where = target(chip, step, chips)
        part = pl.ds(pl.multiple_of(where * chip_rows, chip_rows), chip_rows)
        pairs = ((gradient.at[0, 0], g_buf), (momentum, m_buf), (worker_error.at[0, 0], w_buf))
        three = [
            pltpu.make_async_copy(src.at[part], dst.at[at], sems.at[at, kind]) for kind, (src, dst) in enumerate(pairs)
        ]
        for copy in three:
            copy.start()
        copies.append((where, three))
    brought = [pltpu.make_async_copy(src, dst, small_sems.at[i]) for i, (src, dst) in enumerate(zip(small, near_small))]
    for copy in brought:
        copy.start()
    for at, (where, three) in enumerate(copies):
        for copy in three:
            copy.wait()
        mine = core if order[at] == 0 else 1 - core
        for side, half in enumerate((mine, 1 - mine)):
            some = pl.ds(pl.multiple_of(half * shard_rows, shard_rows), shard_rows)
            local = 0.9 * m_buf[at, some] + 0.1 * g_buf[at, some].astype(jnp.float32) + w_buf[at, some]
            first = packed_of(local, width)
            if side == 0:
                kept[at][...] = first
            elif at == 0:
                sooner[...] = first
            else:
                later[at - 1] = first
            start = pl.multiple_of(where * chip_rows + half * shard_rows, shard_rows)
            error[pl.ds(start, shard_rows), :] = local - first
    for copy in brought:
        copy.wait()


def head(gradient, momentum, worker_error, small, order):
    rows, width = momentum.shape
    chips = len(order)
    chip_rows = rows // chips
    shard = (chip_rows // CORES, width)
    return pl.pallas_call(
        functools.partial(head_kernel, order),
        out_shape=[vmem(*shard)] * (chips + 1) + [vmem(chips - 1, *shard), vmem(rows, width)] + [vmem(*x.shape) for x in small],
        in_specs=[HBM] * 6,
        out_specs=[VMEM] * (chips + 6),
        scratch_shapes=[
            pltpu.VMEM((chips, chip_rows, width), gradient.dtype),
            pltpu.VMEM((chips, chip_rows, width), jnp.float32),
            pltpu.VMEM((chips, chip_rows, width), jnp.float32),
            pltpu.SemaphoreType.DMA((chips, 3)),
            pltpu.SemaphoreType.DMA((3,)),
        ],
        compiler_params=room(gradient.nbytes, momentum.nbytes, worker_error.nbytes),
    )(*far(gradient, momentum, worker_error, *small))


def server_kernel(nodes, count, *refs):
    parts, (server, worker, second, error_0, error_1) = refs[:count], refs[count:]
    width = server.shape[-1]
    total = parts[0][...]
    for other in parts[1:]:
        total = total + other[...]
    values = total / nodes + server[...]
    group_q = packed_of(values, width)
    error_0[...] = values - group_q
    values = group_q + worker[...]
    result = packed_of(values, width)
    second[...] = result
    error_1[...] = values - result


def serve(parts, server, worker, nodes):
    return pl.pallas_call(
        functools.partial(server_kernel, nodes, len(parts)),
        out_shape=[vmem(*server.shape)] * 3,
        in_specs=[VMEM] * (len(parts) + 2),
        out_specs=[VMEM] * 3,
        compiler_params=room(),
    )(*near(*parts, server, worker))


def store_kernel(count, *refs):
    sems = refs[-1]
    copies = [pltpu.make_async_copy(refs[i], refs[count + i], sems.at[i]) for i in range(count)]
    for copy in copies:
        copy.start()
    for copy in copies:
        copy.wait()


def store(*values):
    count = len(values)
    return pl.pallas_call(
        functools.partial(store_kernel, count),
        out_shape=[pltpu.HBM(value.shape, jnp.float32) for value in values],
        in_specs=[VMEM] * count,
        out_specs=[HBM] * count,
        scratch_shapes=[pltpu.SemaphoreType.DMA((count,))],
        compiler_params=room(),
    )(*near(*values))


def average_kernel(order, *refs):
    groups = len(order)
    parts, pieces, (result, error, server) = refs[:groups], refs[groups : 2 * groups], refs[2 * groups :]
    piece_rows, width = pieces[0].shape
    group = lax.axis_index("group")
    for step, piece in zip(order, pieces):
        server[source(group, step, groups)] = piece[...]
    total = parts[0][...]
    for other in parts[1:]:
        total = total + other[...]
    mean = total / groups
    for at in range(groups):
        part = slice(at * piece_rows, (at + 1) * piece_rows)
        values = mean[part] + server[at]
        packed = packed_of(values, width)
        result[part, :] = packed
        error[at] = values - packed


def average(parts, pieces, order):
    groups = len(order)
    stacked = (groups, *pieces[0].shape)
    return pl.pallas_call(
        functools.partial(average_kernel, order),
        out_shape=[vmem(*parts[0].shape), vmem(*stacked)],
        in_specs=[VMEM] * (2 * groups),
        out_specs=[VMEM] * 2,
        scratch_shapes=[pltpu.VMEM(stacked, jnp.float32)],
        compiler_params=room(parts[0].nbytes),
    )(*near(*parts, *pieces))


def first_kernel(chips, mine, given, variance, params, error, new_params, new_momentum, new_error, *scratch):
    own = pltpu.make_async_copy(error.at[lax.axis_index("group")], new_error, scratch[-1])
    own.start()
    update_kernel([0], chips, mine, given, variance, params, new_params, new_momentum, *scratch[:-1])
    own.wait()


def update_first(mine, given, variance, params, error, chips):
    shard_rows, width = mine.shape
    buffer = (1, CORES * shard_rows, width)
    return pl.pallas_call(
        functools.partial(first_kernel, chips),
        out_shape=[pltpu.HBM(params.shape, jnp.float32)] * 2 + [pltpu.HBM(error.shape[1:], jnp.float32)],
        in_specs=[VMEM] * 5,
        out_specs=[HBM] * 3,
        scratch_shapes=[
            pltpu.VMEM(buffer, jnp.float32),
            pltpu.VMEM(buffer, jnp.float32),
            pltpu.SemaphoreType.DMA((1, 2)),
            pltpu.SemaphoreType.DMA,
        ],
        compiler_params=room(2 * CORES * mine.nbytes),
    )(*near(mine, given, variance, params, error))


def update_kernel(steps, chips, *refs):
    count = len(steps)
    mine, given, (variance, params) = refs[:count], refs[count : 2 * count], refs[2 * count : 2 * count + 2]
    new_params, new_momentum, p_buf, m_buf, sems = refs[-5:]
    shard_rows = mine[0].shape[0]
    chip_rows = CORES * shard_rows
    chip, core = place_of()
    copies = []
    for at, step in enumerate(steps):
        part = pl.ds(pl.multiple_of(source(chip, step, chips) * chip_rows, chip_rows), chip_rows)
        half = core if step == 0 else 1 - core
        for values, side in ((mine[at], half), (given[at], 1 - half)):
            m_buf[at, pl.ds(pl.multiple_of(side * shard_rows, shard_rows), shard_rows), :] = values[...]
        copies.append(pltpu.make_async_copy(m_buf.at[at], new_momentum.at[part], sems.at[at, 0]))
        copies[-1].start()
        p_buf[at] = params[part, :] - 0.05 * m_buf[at] / (jnp.sqrt(variance[part, :]) + 1e-08)
        copies.append(pltpu.make_async_copy(p_buf.at[at], new_params.at[part], sems.at[at, 1]))
        copies[-1].start()
    for copy in copies:
        copy.wait()


def update(mine, given, variance, params, so_far, steps, chips):
    shard_rows, width = mine[0].shape
    count = len(steps)
    buffer = (count, CORES * shard_rows, width)
    return pl.pallas_call(
        functools.partial(update_kernel, steps, chips),
        out_shape=[pltpu.HBM(params.shape, jnp.float32)] * 2,
        in_specs=[VMEM] * (2 * count + 2) + [HBM] * len(so_far),
        out_specs=[HBM] * 2,
        scratch_shapes=[
            pltpu.VMEM(buffer, jnp.float32),
            pltpu.VMEM(buffer, jnp.float32),
            pltpu.SemaphoreType.DMA((count, 2)),
        ],
        input_output_aliases={2 * count + 2 + i: i for i in range(len(so_far))},
        compiler_params=room(2 * count * CORES * mine[0].nbytes),
    )(*near(*mine, *given, variance, params), *so_far)


def body(
    gradient,
    momentum,
    variance,
    params,
    worker_error,
    server_error,
    group_worker_error,
    group_server_error,
):
    nodes = lax.axis_size("node")
    groups = lax.axis_size("group")
    chips = nodes // CORES
    along, back, across = farthest_first(chips), farthest_last(chips), farthest_first(groups)

    small = (server_error[0], group_worker_error[0], group_server_error)
    *kept, sooner, later, error, server, worker, own_piece = head(gradient, momentum, worker_error, small, along + [0])
    got = [swap_cores(sooner, nodes)]
    got += list(swap_cores(later, nodes))
    parts = [kept[-1], got[-1]]
    for at, step in enumerate(along):
        parts.append(send_chip(kept[at] + got[at], step, nodes))

    got_pieces = []
    for step in across:
        got_pieces.append(send_group(own_piece, step, groups))

    second, error_0, error_1 = serve(parts, server, worker, nodes)
    seconds = [second]
    for step in across:
        seconds.append(send_group(second, step, groups))
    new_worker_error, new_server_error, new_group_worker_error = store(error[None, None], error_0[None], error_1[None])

    mine, shard_error = average(seconds, [own_piece] + got_pieces, [0] + across)

    arrived = {0: mine}
    for step in back:
        arrived[step] = send_chip(mine, step, nodes)
    order = [0] + back
    given = {}
    for step in order:
        given[step] = swap_cores(arrived[step], nodes)
    *outs, new_group_server_error = update_first(mine, given[0], variance, params, shard_error, chips)
    for some in (order[1:-1], order[-1:]):
        outs = update([arrived[i] for i in some], [given[i] for i in some], variance, params, outs, some, chips)
    new_params, new_momentum = outs
    return (
        new_params,
        new_momentum,
        new_worker_error,
        new_server_error,
        new_group_worker_error,
        new_group_server_error,
    )


def solution(mesh):
    in_specs = (
        P("node", "group", None, None),
        P(),
        P(),
        P(),
        P("node", "group", None, None),
        P("group", "node", None),
        P("group", "node", None),
        P(("node", "group"), None),
    )
    out_specs = (
        P(),
        P(),
        P("node", "group", None, None),
        P("group", "node", None),
        P("group", "node", None),
        P(("node", "group"), None),
    )
    return jax.shard_map(body, mesh=mesh, in_specs=in_specs, out_specs=out_specs, check_vma=False)
```

```python
import functools

import jax
import jax.numpy as jnp
from jax import lax
from jax.experimental import pallas as pl
from jax.experimental.pallas import tpu as pltpu
from jax.sharding import PartitionSpec as P

CORES = 2
VMEM = pl.BlockSpec(memory_space=pltpu.VMEM)
HBM = pl.BlockSpec(memory_space=pltpu.HBM)


def paired(size):
    return size & (size - 1) == 0


def target(index, step, size):
    if paired(size):
        return index ^ step
    return lax.rem(index + step, size) if not isinstance(index, int) else (index + step) % size


def source(index, step, size):
    return index ^ step if paired(size) else lax.rem(index + (size - step), size)


def farthest_first(size):
    return list(range(size - 1, 0, -1))


def farthest_last(size):
    steps = farthest_first(size)
    return steps[1:] + steps[:1]


def crossed_back(step):
    return step > 0 and step % 2 == 0


def packed_of(values, width):
    scale = jnp.sum(jnp.abs(values), axis=-1, keepdims=True) / width
    return jnp.where(values > 0, scale, jnp.where(values < 0, -scale, jnp.zeros_like(values)))


def swap_cores(values, nodes):
    return lax.ppermute(values, "node", [(i, i ^ 1) for i in range(nodes)])


def send_chip(values, step, nodes, crossed):
    chips = nodes // CORES
    pairs = [
        (CORES * i + core, CORES * target(i, step, chips) + (1 - core if crossed else core))
        for i in range(chips)
        for core in range(CORES)
    ]
    return lax.ppermute(values, "node", pairs)


def send_group(values, step, groups):
    return lax.ppermute(values, "group", [(i, target(i, step, groups)) for i in range(groups)])


def vmem(*shape):
    return pltpu.VMEM(shape, jnp.float32)


def near(*values):
    return [pltpu.with_memory_space_constraint(value, pltpu.VMEM) for value in values]


def far(*values):
    return [pltpu.with_memory_space_constraint(value, pltpu.HBM) for value in values]


def room(*scratch):
    return pltpu.CompilerParams(vmem_limit_bytes=sum(scratch) + (4 << 20))


def place_of():
    node = lax.axis_index("node")
    return node // CORES, lax.rem(node, CORES)


def head_kernel(order, joined, gradient, momentum, worker_error, *rest):
    chips = len(order)
    kept, (sooner, later, error, g_buf, m_buf, w_buf, sems) = rest[:chips], rest[chips:]
    rows, width = momentum.shape
    chip_rows = rows // chips
    shard_rows = chip_rows // CORES
    block_rows = joined * chip_rows
    chip, core = place_of()
    blocks = []
    for at in range(0, chips, joined):
        block = target(chip, order[at], chips) // joined
        part = pl.ds(pl.multiple_of(block * block_rows, block_rows), block_rows)
        pairs = ((gradient.at[0, 0], g_buf), (momentum, m_buf), (worker_error.at[0, 0], w_buf))
        three = [
            pltpu.make_async_copy(src.at[part], dst.at[part], sems.at[at // joined, kind])
            for kind, (src, dst) in enumerate(pairs)
        ]
        for copy in three:
            copy.start()
        blocks.append(three)
    for at, step in enumerate(order):
        if at % joined == 0:
            for copy in blocks[at // joined]:
                copy.wait()
        where = target(chip, step, chips)
        mine = 1 - core if step else core
        for side, half in enumerate((mine, 1 - mine)):
            some = pl.ds(pl.multiple_of(where * chip_rows + half * shard_rows, shard_rows), shard_rows)
            local = 0.9 * m_buf[some, :] + 0.1 * g_buf[some, :].astype(jnp.float32) + w_buf[some, :]
            first = packed_of(local, width)
            if side == 0:
                kept[at][...] = first
            elif at == 0:
                sooner[...] = first
            else:
                later[at - 1] = first
            error[some, :] = local - first


def head(gradient, momentum, worker_error, order):
    rows, width = momentum.shape
    chips = len(order)
    shard = (rows // chips // CORES, width)
    joined = 2 if paired(chips) and chips % 2 == 0 else 1
    return pl.pallas_call(
        functools.partial(head_kernel, order, joined),
        out_shape=[vmem(*shard)] * (chips + 1) + [vmem(chips - 1, *shard), vmem(rows, width)],
        in_specs=[HBM] * 3,
        out_specs=[VMEM] * (chips + 3),
        scratch_shapes=[
            pltpu.VMEM((rows, width), gradient.dtype),
            pltpu.VMEM((rows, width), jnp.float32),
            pltpu.VMEM((rows, width), jnp.float32),
            pltpu.SemaphoreType.DMA((chips // joined, 3)),
        ],
        compiler_params=room(gradient.nbytes, momentum.nbytes, worker_error.nbytes),
    )(*far(gradient, momentum, worker_error))


def server_kernel(nodes, groups, count, *refs):
    parts, (server, worker, piece, second, error_0, error_1) = refs[:count], refs[count:]
    width = server.shape[-1]
    piece_rows = piece.shape[0]
    total = parts[0][...]
    for other in parts[1:]:
        total = total + other[...]
    values = total / nodes + server[...]
    group_q = packed_of(values, width)
    error_0[...] = values - group_q
    values = group_q + worker[...]
    result = packed_of(values, width)
    error_1[...] = values - result
    group = lax.axis_index("group")
    for at in range(groups):
        part = slice(at * piece_rows, (at + 1) * piece_rows)
        second[part, :] = result[part] + jnp.where(group == at, groups * piece[...], jnp.zeros_like(piece))


def serve(parts, server, worker, piece, nodes, groups):
    return pl.pallas_call(
        functools.partial(server_kernel, nodes, groups, len(parts)),
        out_shape=[vmem(*server.shape)] * 3,
        in_specs=[VMEM] * (len(parts) + 3),
        out_specs=[VMEM] * 3,
        compiler_params=room(),
    )(*near(*parts, server, worker, piece))


def store_kernel(count, *refs):
    sems = refs[-1]
    copies = [pltpu.make_async_copy(refs[i], refs[count + i], sems.at[i]) for i in range(count)]
    for copy in copies:
        copy.start()
    for copy in copies:
        copy.wait()


def store(*values):
    count = len(values)
    return pl.pallas_call(
        functools.partial(store_kernel, count),
        out_shape=[pltpu.HBM(value.shape, jnp.float32) for value in values],
        in_specs=[VMEM] * count,
        out_specs=[HBM] * count,
        scratch_shapes=[pltpu.SemaphoreType.DMA((count,))],
        compiler_params=room(),
    )(*near(*values))


def average_kernel(groups, *refs):
    parts, (result, error) = refs[:groups], refs[groups:]
    piece_rows, width = error.shape[1:]
    total = parts[0][...]
    for other in parts[1:]:
        total = total + other[...]
    values = total / groups
    packed = packed_of(values, width)
    result[...] = packed
    for at in range(groups):
        part = slice(at * piece_rows, (at + 1) * piece_rows)
        error[at] = values[part] - packed[part]


def average(parts):
    groups = len(parts)
    rows, width = parts[0].shape
    return pl.pallas_call(
        functools.partial(average_kernel, groups),
        out_shape=[vmem(rows, width), vmem(groups, rows // groups, width)],
        in_specs=[VMEM] * groups,
        out_specs=[VMEM] * 2,
        compiler_params=room(),
    )(*near(*parts))


def first_kernel(chips, mine, given, variance, params, error, new_params, new_momentum, new_error, *scratch):
    own = pltpu.make_async_copy(error.at[lax.axis_index("group")], new_error, scratch[-1])
    own.start()
    update_kernel([0], chips, mine, given, variance, params, new_params, new_momentum, *scratch[:-1])
    own.wait()


def update_first(mine, given, variance, params, error, chips):
    shard_rows, width = mine.shape
    buffer = (1, CORES * shard_rows, width)
    return pl.pallas_call(
        functools.partial(first_kernel, chips),
        out_shape=[pltpu.HBM(params.shape, jnp.float32)] * 2 + [pltpu.HBM(error.shape[1:], jnp.float32)],
        in_specs=[VMEM] * 5,
        out_specs=[HBM] * 3,
        scratch_shapes=[
            pltpu.VMEM(buffer, jnp.float32),
            pltpu.VMEM(buffer, jnp.float32),
            pltpu.SemaphoreType.DMA((1, 2)),
            pltpu.SemaphoreType.DMA,
        ],
        compiler_params=room(2 * CORES * mine.nbytes),
    )(*near(mine, given, variance, params, error))


def update_kernel(steps, chips, *refs):
    count = len(steps)
    mine, given, (variance, params) = refs[:count], refs[count : 2 * count], refs[2 * count : 2 * count + 2]
    new_params, new_momentum, p_buf, m_buf, sems = refs[-5:]
    shard_rows = mine[0].shape[0]
    chip_rows = CORES * shard_rows
    chip, core = place_of()
    copies = []
    for at, step in enumerate(steps):
        part = pl.ds(pl.multiple_of(source(chip, step, chips) * chip_rows, chip_rows), chip_rows)
        half = 1 - core if crossed_back(step) else core
        for values, side in ((mine[at], half), (given[at], 1 - half)):
            m_buf[at, pl.ds(pl.multiple_of(side * shard_rows, shard_rows), shard_rows), :] = values[...]
        copies.append(pltpu.make_async_copy(m_buf.at[at], new_momentum.at[part], sems.at[at, 0]))
        copies[-1].start()
        p_buf[at] = params[part, :] - 0.05 * m_buf[at] / (jnp.sqrt(variance[part, :]) + 1e-08)
        copies.append(pltpu.make_async_copy(p_buf.at[at], new_params.at[part], sems.at[at, 1]))
        copies[-1].start()
    for copy in copies:
        copy.wait()


def update(mine, given, variance, params, so_far, steps, chips):
    shard_rows, width = mine[0].shape
    count = len(steps)
    buffer = (count, CORES * shard_rows, width)
    return pl.pallas_call(
        functools.partial(update_kernel, steps, chips),
        out_shape=[pltpu.HBM(params.shape, jnp.float32)] * 2,
        in_specs=[VMEM] * (2 * count + 2) + [HBM] * len(so_far),
        out_specs=[HBM] * 2,
        scratch_shapes=[
            pltpu.VMEM(buffer, jnp.float32),
            pltpu.VMEM(buffer, jnp.float32),
            pltpu.SemaphoreType.DMA((count, 2)),
        ],
        input_output_aliases={2 * count + 2 + i: i for i in range(len(so_far))},
        compiler_params=room(2 * count * CORES * mine[0].nbytes),
    )(*near(*mine, *given, variance, params), *so_far)


def body(
    gradient,
    momentum,
    variance,
    params,
    worker_error,
    server_error,
    group_worker_error,
    group_server_error,
):
    nodes = lax.axis_size("node")
    groups = lax.axis_size("group")
    chips = nodes // CORES
    along, back, across = farthest_first(chips), farthest_last(chips), farthest_first(groups)

    *kept, sooner, later, error = head(gradient, momentum, worker_error, along + [0])
    got = [swap_cores(sooner, nodes)]
    got += list(swap_cores(later, nodes))
    parts = [kept[-1], got[-1]]
    for at, step in enumerate(along):
        parts.append(send_chip(kept[at] + got[at], step, nodes, True))

    second, error_0, error_1 = serve(parts, server_error[0], group_worker_error[0], group_server_error, nodes, groups)
    seconds = [second]
    for step in across:
        seconds.append(send_group(second, step, groups))
    new_worker_error, new_server_error, new_group_worker_error = store(error[None, None], error_0[None], error_1[None])

    mine, shard_error = average(seconds)

    arrived = {0: mine}
    for step in back:
        arrived[step] = send_chip(mine, step, nodes, crossed_back(step))
    order = [0] + back
    given = {}
    for step in order:
        given[step] = swap_cores(arrived[step], nodes)
    *outs, new_group_server_error = update_first(mine, given[0], variance, params, shard_error, chips)
    for some in (order[1:-1], order[-1:]):
        outs = update([arrived[i] for i in some], [given[i] for i in some], variance, params, outs, some, chips)
    new_params, new_momentum = outs
    return (
        new_params,
        new_momentum,
        new_worker_error,
        new_server_error,
        new_group_worker_error,
        new_group_server_error,
    )


def solution(mesh):
    in_specs = (
        P("node", "group", None, None),
        P(),
        P(),
        P(),
        P("node", "group", None, None),
        P("group", "node", None),
        P("group", "node", None),
        P(("node", "group"), None),
    )
    out_specs = (
        P(),
        P(),
        P("node", "group", None, None),
        P("group", "node", None),
        P("group", "node", None),
        P(("node", "group"), None),
    )
    return jax.shard_map(body, mesh=mesh, in_specs=in_specs, out_specs=out_specs, check_vma=False)
```

```python
import functools

import jax
import jax.numpy as jnp
from jax import lax
from jax.experimental import pallas as pl
from jax.experimental.pallas import tpu as pltpu
from jax.sharding import PartitionSpec as P

CORES = 2
VMEM = pl.BlockSpec(memory_space=pltpu.VMEM)
HBM = pl.BlockSpec(memory_space=pltpu.HBM)


def paired(size):
    return size & (size - 1) == 0


def target(index, step, size):
    if paired(size):
        return index ^ step
    return lax.rem(index + step, size) if not isinstance(index, int) else (index + step) % size


def source(index, step, size):
    return index ^ step if paired(size) else lax.rem(index + (size - step), size)


def farthest_first(size):
    return list(range(size - 1, 0, -1))


def farthest_last(size):
    steps = farthest_first(size)
    return steps[1:] + steps[:1]


def crossed_back(step):
    return step > 0 and step % 2 == 0


def packed_of(values, width):
    scale = jnp.sum(jnp.abs(values), axis=-1, keepdims=True) / width
    return jnp.where(values > 0, scale, jnp.where(values < 0, -scale, jnp.zeros_like(values)))


def swap_cores(values, nodes):
    return lax.ppermute(values, "node", [(i, i ^ 1) for i in range(nodes)])


def send_chip(values, step, nodes, crossed):
    chips = nodes // CORES
    pairs = [
        (CORES * i + core, CORES * target(i, step, chips) + (1 - core if crossed else core))
        for i in range(chips)
        for core in range(CORES)
    ]
    return lax.ppermute(values, "node", pairs)


def send_group(values, steps, nodes, groups):
    pairs = [
        (i * groups + j, i * groups + target(j, steps[i % CORES], groups)) for i in range(nodes) for j in range(groups)
    ]
    return lax.ppermute(values, ("node", "group"), pairs)


def turns(steps):
    return list(zip(steps[:-2] + steps[-2:][::-1], steps))


def vmem(*shape):
    return pltpu.VMEM(shape, jnp.float32)


def near(*values):
    return [pltpu.with_memory_space_constraint(value, pltpu.VMEM) for value in values]


def far(*values):
    return [pltpu.with_memory_space_constraint(value, pltpu.HBM) for value in values]


def room(*scratch):
    return pltpu.CompilerParams(vmem_limit_bytes=sum(scratch) + (4 << 20))


def place_of():
    node = lax.axis_index("node")
    return node // CORES, lax.rem(node, CORES)


def head_kernel(order, joined, gradient, momentum, worker_error, *rest):
    chips = len(order)
    kept, (sooner, later, error, g_buf, m_buf, w_buf, sems) = rest[:chips], rest[chips:]
    rows, width = momentum.shape
    chip_rows = rows // chips
    shard_rows = chip_rows // CORES
    block_rows = joined * chip_rows
    chip, core = place_of()
    blocks = []
    for at in range(0, chips, joined):
        block = target(chip, order[at], chips) // joined
        part = pl.ds(pl.multiple_of(block * block_rows, block_rows), block_rows)
        pairs = ((gradient.at[0, 0], g_buf), (momentum, m_buf), (worker_error.at[0, 0], w_buf))
        three = [
            pltpu.make_async_copy(src.at[part], dst.at[part], sems.at[at // joined, kind])
            for kind, (src, dst) in enumerate(pairs)
        ]
        for copy in three:
            copy.start()
        blocks.append(three)
    for at, step in enumerate(order):
        if at % joined == 0:
            for copy in blocks[at // joined]:
                copy.wait()
        where = target(chip, step, chips)
        mine = 1 - core if step else core
        for side, half in enumerate((mine, 1 - mine)):
            some = pl.ds(pl.multiple_of(where * chip_rows + half * shard_rows, shard_rows), shard_rows)
            local = 0.9 * m_buf[some, :] + 0.1 * g_buf[some, :].astype(jnp.float32) + w_buf[some, :]
            first = packed_of(local, width)
            if side == 0:
                kept[at][...] = first
            elif at == 0:
                sooner[...] = first
            else:
                later[at - 1] = first
            error[some, :] = local - first


def head(gradient, momentum, worker_error, order):
    rows, width = momentum.shape
    chips = len(order)
    shard = (rows // chips // CORES, width)
    joined = 2 if paired(chips) and chips % 2 == 0 else 1
    return pl.pallas_call(
        functools.partial(head_kernel, order, joined),
        out_shape=[vmem(*shard)] * (chips + 1) + [vmem(chips - 1, *shard), vmem(rows, width)],
        in_specs=[HBM] * 3,
        out_specs=[VMEM] * (chips + 3),
        scratch_shapes=[
            pltpu.VMEM((rows, width), gradient.dtype),
            pltpu.VMEM((rows, width), jnp.float32),
            pltpu.VMEM((rows, width), jnp.float32),
            pltpu.SemaphoreType.DMA((chips // joined, 3)),
        ],
        compiler_params=room(gradient.nbytes, momentum.nbytes, worker_error.nbytes),
    )(*far(gradient, momentum, worker_error))


def server_kernel(nodes, groups, count, *refs):
    parts, (server, worker, piece, second, error_0, error_1) = refs[:count], refs[count:]
    width = server.shape[-1]
    piece_rows = piece.shape[0]
    total = parts[0][...]
    for other in parts[1:]:
        total = total + other[...]
    values = total / nodes + server[...]
    group_q = packed_of(values, width)
    error_0[...] = values - group_q
    values = group_q + worker[...]
    result = packed_of(values, width)
    error_1[...] = values - result
    group = lax.axis_index("group")
    for at in range(groups):
        part = slice(at * piece_rows, (at + 1) * piece_rows)
        second[part, :] = result[part] + jnp.where(group == at, groups * piece[...], jnp.zeros_like(piece))


def serve(parts, server, worker, piece, nodes, groups):
    return pl.pallas_call(
        functools.partial(server_kernel, nodes, groups, len(parts)),
        out_shape=[vmem(*server.shape)] * 3,
        in_specs=[VMEM] * (len(parts) + 3),
        out_specs=[VMEM] * 3,
        compiler_params=room(),
    )(*near(*parts, server, worker, piece))


def store_kernel(count, *refs):
    sems = refs[-1]
    copies = [pltpu.make_async_copy(refs[i], refs[count + i], sems.at[i]) for i in range(count)]
    for copy in copies:
        copy.start()
    for copy in copies:
        copy.wait()


def store(*values):
    count = len(values)
    return pl.pallas_call(
        functools.partial(store_kernel, count),
        out_shape=[pltpu.HBM(value.shape, jnp.float32) for value in values],
        in_specs=[VMEM] * count,
        out_specs=[HBM] * count,
        scratch_shapes=[pltpu.SemaphoreType.DMA((count,))],
        compiler_params=room(),
    )(*near(*values))


def average_kernel(groups, *refs):
    parts, (result, error) = refs[:groups], refs[groups:]
    piece_rows, width = error.shape[1:]
    total = parts[0][...]
    for other in parts[1:]:
        total = total + other[...]
    values = total / groups
    packed = packed_of(values, width)
    result[...] = packed
    for at in range(groups):
        part = slice(at * piece_rows, (at + 1) * piece_rows)
        error[at] = values[part] - packed[part]


def average(parts):
    groups = len(parts)
    rows, width = parts[0].shape
    return pl.pallas_call(
        functools.partial(average_kernel, groups),
        out_shape=[vmem(rows, width), vmem(groups, rows // groups, width)],
        in_specs=[VMEM] * groups,
        out_specs=[VMEM] * 2,
        compiler_params=room(),
    )(*near(*parts))


def update_rows(items, chips, values, variance, params, new_params, new_momentum, p_buf, sems):
    shard_rows = values[0].shape[0]
    chip, core = place_of()
    copies = []
    for at, (step, given) in enumerate(items):
        half = core if crossed_back(step) == given else 1 - core
        start = (source(chip, step, chips) * CORES + half) * shard_rows
        part = pl.ds(pl.multiple_of(start, shard_rows), shard_rows)
        copies.append(pltpu.make_async_copy(values[at], new_momentum.at[part], sems.at[at, 0]))
        copies[-1].start()
        p_buf[at] = params[part, :] - 0.05 * values[at][...] / (jnp.sqrt(variance[part, :]) + 1e-08)
        copies.append(pltpu.make_async_copy(p_buf.at[at], new_params.at[part], sems.at[at, 1]))
        copies[-1].start()
    return copies


def update_kernel(items, chips, *refs):
    count = len(items)
    for copy in update_rows(items, chips, refs[:count], *refs[count : count + 2], *refs[-4:]):
        copy.wait()


def update(values, variance, params, so_far, items, chips):
    count = len(items)
    return pl.pallas_call(
        functools.partial(update_kernel, items, chips),
        out_shape=[pltpu.HBM(params.shape, jnp.float32)] * 2,
        in_specs=[VMEM] * (count + 2) + [HBM] * len(so_far),
        out_specs=[HBM] * 2,
        scratch_shapes=[
            pltpu.VMEM((count, *values[0].shape), jnp.float32),
            pltpu.SemaphoreType.DMA((count, 2)),
        ],
        input_output_aliases={count + 2 + i: i for i in range(len(so_far))},
        compiler_params=room(count * values[0].nbytes),
    )(*near(*values, variance, params), *so_far)


def first_kernel(items, chips, mine, given, variance, params, error, *rest):
    new_params, new_momentum, new_error, p_buf, sems, error_sem = rest
    own = pltpu.make_async_copy(error.at[lax.axis_index("group")], new_error, error_sem)
    own.start()
    outs = (new_params, new_momentum, p_buf, sems)
    for copy in update_rows(items, chips, (mine, given), variance, params, *outs) + [own]:
        copy.wait()


def update_first(mine, given, variance, params, error, chips):
    items = [(0, False), (0, True)]
    return pl.pallas_call(
        functools.partial(first_kernel, items, chips),
        out_shape=[pltpu.HBM(params.shape, jnp.float32)] * 2 + [pltpu.HBM(error.shape[1:], jnp.float32)],
        in_specs=[VMEM] * 5,
        out_specs=[HBM] * 3,
        scratch_shapes=[
            pltpu.VMEM((len(items), *mine.shape), jnp.float32),
            pltpu.SemaphoreType.DMA((len(items), 2)),
            pltpu.SemaphoreType.DMA,
        ],
        compiler_params=room(len(items) * mine.nbytes),
    )(*near(mine, given, variance, params, error))


def body(
    gradient,
    momentum,
    variance,
    params,
    worker_error,
    server_error,
    group_worker_error,
    group_server_error,
):
    nodes = lax.axis_size("node")
    groups = lax.axis_size("group")
    chips = nodes // CORES
    along, back, across = farthest_first(chips), farthest_last(chips), farthest_first(groups)

    *kept, sooner, later, error = head(gradient, momentum, worker_error, along + [0])
    got = [swap_cores(sooner, nodes)]
    got += list(swap_cores(later, nodes))
    parts = [kept[-1], got[-1]]
    for at, step in enumerate(along):
        parts.append(send_chip(kept[at] + got[at], step, nodes, True))

    second, error_0, error_1 = serve(parts, server_error[0], group_worker_error[0], group_server_error, nodes, groups)
    seconds = [second]
    for step, both in zip(across, turns(across)):
        seconds.append(send_group(second, both, nodes, groups))
    new_worker_error, new_server_error, new_group_worker_error = store(error[None, None], error_0[None], error_1[None])

    mine, shard_error = average(seconds)

    arrived = {0: mine}
    for step in back:
        arrived[step] = send_chip(mine, step, nodes, crossed_back(step))
    order = [0] + back
    given = {}
    for step in order:
        given[step] = swap_cores(arrived[step], nodes)
    *outs, new_group_server_error = update_first(mine, given[0], variance, params, shard_error, chips)
    items = [(step, here) for step in order[1:] for here in (False, True)]
    for some in (items[:-1], items[-1:]):
        values = [given[step] if here else arrived[step] for step, here in some]
        outs = update(values, variance, params, outs, some, chips)
    new_params, new_momentum = outs
    return (
        new_params,
        new_momentum,
        new_worker_error,
        new_server_error,
        new_group_worker_error,
        new_group_server_error,
    )


def solution(mesh):
    in_specs = (
        P("node", "group", None, None),
        P(),
        P(),
        P(),
        P("node", "group", None, None),
        P("group", "node", None),
        P("group", "node", None),
        P(("node", "group"), None),
    )
    out_specs = (
        P(),
        P(),
        P("node", "group", None, None),
        P("group", "node", None),
        P("group", "node", None),
        P(("node", "group"), None),
    )
    return jax.shard_map(body, mesh=mesh, in_specs=in_specs, out_specs=out_specs, check_vma=False)
```

```python
import functools

import jax
import jax.numpy as jnp
from jax import lax
from jax.experimental import pallas as pl
from jax.experimental.pallas import tpu as pltpu
from jax.sharding import PartitionSpec as P

CORES = 2
VMEM = pl.BlockSpec(memory_space=pltpu.VMEM)
HBM = pl.BlockSpec(memory_space=pltpu.HBM)


def paired(size):
    return size & (size - 1) == 0


def target(index, step, size):
    if paired(size):
        return index ^ step
    return lax.rem(index + step, size) if not isinstance(index, int) else (index + step) % size


def source(index, step, size):
    return index ^ step if paired(size) else lax.rem(index + (size - step), size)


def farthest_first(size):
    return list(range(size - 1, 0, -1))


def farthest_last(size):
    steps = farthest_first(size)
    return steps[1:] + steps[:1]


def crossed_back(step):
    return step > 0 and step % 2 == 0


def packed_of(values, width):
    scale = jnp.sum(jnp.abs(values), axis=-1, keepdims=True) / width
    return jnp.where(values > 0, scale, jnp.where(values < 0, -scale, jnp.zeros_like(values)))


def swap_cores(values, nodes):
    return lax.ppermute(values, "node", [(i, i ^ 1) for i in range(nodes)])


def send_chip(values, step, nodes, crossed):
    chips = nodes // CORES
    pairs = [
        (CORES * i + core, CORES * target(i, step, chips) + (1 - core if crossed else core))
        for i in range(chips)
        for core in range(CORES)
    ]
    return lax.ppermute(values, "node", pairs)


def send_group(values, step, groups):
    return lax.ppermute(values, "group", [(i, target(i, step, groups)) for i in range(groups)])


def vmem(*shape):
    return pltpu.VMEM(shape, jnp.float32)


def near(*values):
    return [pltpu.with_memory_space_constraint(value, pltpu.VMEM) for value in values]


def far(*values):
    return [pltpu.with_memory_space_constraint(value, pltpu.HBM) for value in values]


def room(*scratch):
    return pltpu.CompilerParams(vmem_limit_bytes=sum(scratch) + (4 << 20))


def place_of():
    node = lax.axis_index("node")
    return node // CORES, lax.rem(node, CORES)


def head_kernel(order, joined, gradient, momentum, worker_error, *rest):
    chips = len(order)
    kept, (sooner, later, error, g_buf, m_buf, w_buf, sems) = rest[:chips], rest[chips:]
    rows, width = momentum.shape
    chip_rows = rows // chips
    shard_rows = chip_rows // CORES
    block_rows = joined * chip_rows
    chip, core = place_of()
    blocks = []
    for at in range(0, chips, joined):
        block = target(chip, order[at], chips) // joined
        part = pl.ds(pl.multiple_of(block * block_rows, block_rows), block_rows)
        pairs = ((gradient.at[0, 0], g_buf), (momentum, m_buf), (worker_error.at[0, 0], w_buf))
        three = [
            pltpu.make_async_copy(src.at[part], dst.at[part], sems.at[at // joined, kind])
            for kind, (src, dst) in enumerate(pairs)
        ]
        for copy in three:
            copy.start()
        blocks.append(three)
    for at, step in enumerate(order):
        if at % joined == 0:
            for copy in blocks[at // joined]:
                copy.wait()
        where = target(chip, step, chips)
        mine = 1 - core if step else core
        for side, half in enumerate((mine, 1 - mine)):
            some = pl.ds(pl.multiple_of(where * chip_rows + half * shard_rows, shard_rows), shard_rows)
            local = 0.9 * m_buf[some, :] + 0.1 * g_buf[some, :].astype(jnp.float32) + w_buf[some, :]
            first = packed_of(local, width)
            if side == 0:
                kept[at][...] = first
            elif at == 0:
                sooner[...] = first
            else:
                later[at - 1] = first
            error[some, :] = local - first


def head(gradient, momentum, worker_error, order):
    rows, width = momentum.shape
    chips = len(order)
    shard = (rows // chips // CORES, width)
    joined = 2 if paired(chips) and chips % 2 == 0 else 1
    return pl.pallas_call(
        functools.partial(head_kernel, order, joined),
        out_shape=[vmem(*shard)] * (chips + 1) + [vmem(chips - 1, *shard), vmem(rows, width)],
        in_specs=[HBM] * 3,
        out_specs=[VMEM] * (chips + 3),
        scratch_shapes=[
            pltpu.VMEM((rows, width), gradient.dtype),
            pltpu.VMEM((rows, width), jnp.float32),
            pltpu.VMEM((rows, width), jnp.float32),
            pltpu.SemaphoreType.DMA((chips // joined, 3)),
        ],
        compiler_params=room(gradient.nbytes, momentum.nbytes, worker_error.nbytes),
    )(*far(gradient, momentum, worker_error))


def server_kernel(nodes, groups, count, *refs):
    parts, (server, worker, piece, second, error_0, error_1) = refs[:count], refs[count:]
    width = server.shape[-1]
    piece_rows = piece.shape[0]
    total = parts[0][...]
    for other in parts[1:]:
        total = total + other[...]
    values = total / nodes + server[...]
    group_q = packed_of(values, width)
    error_0[...] = values - group_q
    values = group_q + worker[...]
    result = packed_of(values, width)
    error_1[...] = values - result
    group = lax.axis_index("group")
    for at in range(groups):
        part = slice(at * piece_rows, (at + 1) * piece_rows)
        second[part, :] = result[part] + jnp.where(group == at, groups * piece[...], jnp.zeros_like(piece))


def serve(parts, server, worker, piece, nodes, groups):
    return pl.pallas_call(
        functools.partial(server_kernel, nodes, groups, len(parts)),
        out_shape=[vmem(*server.shape)] * 3,
        in_specs=[VMEM] * (len(parts) + 3),
        out_specs=[VMEM] * 3,
        compiler_params=room(),
    )(*near(*parts, server, worker, piece))


def store_kernel(count, *refs):
    sems = refs[-1]
    copies = [pltpu.make_async_copy(refs[i], refs[count + i], sems.at[i]) for i in range(count)]
    for copy in copies:
        copy.start()
    for copy in copies:
        copy.wait()


def store(*values):
    count = len(values)
    return pl.pallas_call(
        functools.partial(store_kernel, count),
        out_shape=[pltpu.HBM(value.shape, jnp.float32) for value in values],
        in_specs=[VMEM] * count,
        out_specs=[HBM] * count,
        scratch_shapes=[pltpu.SemaphoreType.DMA((count,))],
        compiler_params=room(),
    )(*near(*values))


def average_kernel(groups, *refs):
    parts, (result, error) = refs[:groups], refs[groups:]
    piece_rows, width = error.shape[1:]
    total = parts[0][...]
    for other in parts[1:]:
        total = total + other[...]
    values = total / groups
    packed = packed_of(values, width)
    result[...] = packed
    for at in range(groups):
        part = slice(at * piece_rows, (at + 1) * piece_rows)
        error[at] = values[part] - packed[part]


def average(parts):
    groups = len(parts)
    rows, width = parts[0].shape
    return pl.pallas_call(
        functools.partial(average_kernel, groups),
        out_shape=[vmem(rows, width), vmem(groups, rows // groups, width)],
        in_specs=[VMEM] * groups,
        out_specs=[VMEM] * 2,
        compiler_params=room(),
    )(*near(*parts))


def update_rows(items, chips, values, variance, params, new_params, new_momentum, p_buf, sems):
    shard_rows = values[0].shape[0]
    chip, core = place_of()
    copies = []
    for at, (step, given) in enumerate(items):
        half = core if crossed_back(step) == given else 1 - core
        start = (source(chip, step, chips) * CORES + half) * shard_rows
        part = pl.ds(pl.multiple_of(start, shard_rows), shard_rows)
        copies.append(pltpu.make_async_copy(values[at], new_momentum.at[part], sems.at[at, 0]))
        copies[-1].start()
        p_buf[at] = params[part, :] - 0.05 * values[at][...] / (jnp.sqrt(variance[part, :]) + 1e-08)
        copies.append(pltpu.make_async_copy(p_buf.at[at], new_params.at[part], sems.at[at, 1]))
        copies[-1].start()
    return copies


def update_kernel(items, chips, *refs):
    count = len(items)
    for copy in update_rows(items, chips, refs[:count], *refs[count : count + 2], *refs[-4:]):
        copy.wait()


def update(values, variance, params, so_far, items, chips):
    count = len(items)
    return pl.pallas_call(
        functools.partial(update_kernel, items, chips),
        out_shape=[pltpu.HBM(params.shape, jnp.float32)] * 2,
        in_specs=[VMEM] * (count + 2) + [HBM] * len(so_far),
        out_specs=[HBM] * 2,
        scratch_shapes=[
            pltpu.VMEM((count, *values[0].shape), jnp.float32),
            pltpu.SemaphoreType.DMA((count, 2)),
        ],
        input_output_aliases={count + 2 + i: i for i in range(len(so_far))},
        compiler_params=room(count * values[0].nbytes),
    )(*near(*values, variance, params), *so_far)


def first_kernel(items, chips, mine, given, variance, params, error, *rest):
    new_params, new_momentum, new_error, p_buf, sems, error_sem = rest
    own = pltpu.make_async_copy(error.at[lax.axis_index("group")], new_error, error_sem)
    own.start()
    outs = (new_params, new_momentum, p_buf, sems)
    for copy in update_rows(items, chips, (mine, given), variance, params, *outs) + [own]:
        copy.wait()


def update_first(mine, given, variance, params, error, chips):
    items = [(0, False), (0, True)]
    return pl.pallas_call(
        functools.partial(first_kernel, items, chips),
        out_shape=[pltpu.HBM(params.shape, jnp.float32)] * 2 + [pltpu.HBM(error.shape[1:], jnp.float32)],
        in_specs=[VMEM] * 5,
        out_specs=[HBM] * 3,
        scratch_shapes=[
            pltpu.VMEM((len(items), *mine.shape), jnp.float32),
            pltpu.SemaphoreType.DMA((len(items), 2)),
            pltpu.SemaphoreType.DMA,
        ],
        compiler_params=room(len(items) * mine.nbytes),
    )(*near(mine, given, variance, params, error))


def body(
    gradient,
    momentum,
    variance,
    params,
    worker_error,
    server_error,
    group_worker_error,
    group_server_error,
):
    nodes = lax.axis_size("node")
    groups = lax.axis_size("group")
    chips = nodes // CORES
    along, back, across = farthest_first(chips), farthest_last(chips), farthest_first(groups)

    *kept, sooner, later, error = head(gradient, momentum, worker_error, along + [0])
    got = [swap_cores(sooner, nodes)]
    got += list(swap_cores(later, nodes))
    parts = [kept[-1], got[-1]]
    for at, step in enumerate(along):
        parts.append(send_chip(kept[at] + got[at], step, nodes, True))

    second, error_0, error_1 = serve(
        parts, server_error[0], group_worker_error[0], group_server_error, nodes, groups
    )
    seconds = [second]
    for step in across:
        seconds.append(send_group(second, step, groups))
    new_worker_error, new_server_error, new_group_worker_error = store(
        error[None, None], error_0[None], error_1[None]
    )

    mine, shard_error = average(seconds)

    arrived = {0: mine}
    for step in back:
        arrived[step] = send_chip(mine, step, nodes, crossed_back(step))
    order = [0] + sorted(back)
    given = {}
    for step in order:
        given[step] = swap_cores(arrived[step], nodes)
    *outs, new_group_server_error = update_first(mine, given[0], variance, params, shard_error, chips)
    items = [(step, here) for step in order[1:] for here in (False, True)]
    for some in (items[:-1], items[-1:]):
        values = [given[step] if here else arrived[step] for step, here in some]
        outs = update(values, variance, params, outs, some, chips)
    new_params, new_momentum = outs
    return (
        new_params,
        new_momentum,
        new_worker_error,
        new_server_error,
        new_group_worker_error,
        new_group_server_error,
    )


def solution(mesh):
    in_specs = (
        P("node", "group", None, None),
        P(),
        P(),
        P(),
        P("node", "group", None, None),
        P("group", "node", None),
        P("group", "node", None),
        P(("node", "group"), None),
    )
    out_specs = (
        P(),
        P(),
        P("node", "group", None, None),
        P("group", "node", None),
        P("group", "node", None),
        P(("node", "group"), None),
    )
    return jax.shard_map(body, mesh=mesh, in_specs=in_specs, out_specs=out_specs, check_vma=False)
```
